256 devices in a mesh: row: 32 (over y, z_lo, core), col: 8 (over z_hi, x).
Axes of the slice: x: 4, y: 4, z: 8 (z_hi: 2, z_lo: 4; z = z_hi * 4 + z_lo), core: 2. Of those that a mesh axis runs over, the one named last changes fastest.
Arguments:
- left: bfloat16 [16384, 16384], P('row', 'col'), may hold values from -6 to 6
- right: bfloat16 [16384, 16384], P('row', 'col'), may hold values from -0.125 to 0.125
Outputs:
- product: bfloat16 [16384, 16384], P('row', 'col')
The draws below stay inside these ranges and needn't reach their ends.
All inputs are finite; a program needn't handle non-finite values.
Results may differ from the reference program's by a relative error of at most 0.001.
Values may be sent and summed in bfloat16 or wider, within the bound.
No kernel may reach another device: no remote copies, remote signals or barrier semaphores. Data moves between devices by JAX's collectives and lax.ppermute only.
A program may use at most 64 MiB of HBM per device.

```python
import jax
import jax.numpy as jnp
from jax import lax

N = 16384
STEPS = 4
GRID = 32
KB = 512


def steps_of(stream_key, shape, split, least, largest):
    factor_of, own = 1.0, jax.random.fold_in(stream_key, 6)
    for axis_at, shards_of in split:
        steps = jnp.exp(jax.random.uniform(jax.random.fold_in(own, axis_at), (shards_of,), jnp.float32, least / len(split), largest / len(split)))
        factor_of = factor_of * jnp.repeat(steps, shape[axis_at] // shards_of).reshape([-1 if axis == axis_at else 1 for axis in range(len(shape))])
    return factor_of


def scatter_about(rng, extent, spread, bound, split=(), kind=jnp.bfloat16):
    result = jax.random.normal(rng, extent, jnp.float32) * spread
    if len(split) > 0:
        result = steps_of(rng, extent, split, -0.22, 0.18) * result
    return jnp.clip(result, min=-bound, max=bound).astype(kind)


def setup_inputs(seed: int = 0) -> dict:
    key_list = jax.random.split(jax.random.key(seed), 3)
    return {
        "left": scatter_about(key_list[0], (N, N), 1.0, 6.0, ((0, 32), (1, 8))),
        "right": scatter_about(key_list[1], (N, N), (STEPS * KB) ** -0.5, 0.125, ((0, 32), (1, 8))),
    }


def reference(left, right):
    def block_row(index):
        total = jnp.zeros((KB, N), jnp.float32)
        for offset in range(STEPS):
            kblock = (index + offset) % GRID
            piece = lax.dynamic_slice(left, (index * KB, kblock * KB), (KB, KB))
            rows = lax.dynamic_slice_in_dim(right, kblock * KB, KB, 0)
            total = total + jnp.dot(piece, rows, preferred_element_type=jnp.float32)
        return total.astype(jnp.bfloat16)

    blocks = lax.map(block_row, jnp.arange(GRID, dtype=jnp.int32))
    return blocks.reshape(N, N)
```

```python
import jax
import jax.numpy as jnp
from jax import lax
from jax.sharding import PartitionSpec as P


STEPS = 4
HALVES = 2
CHUNKS = 2


def routes(rows, cols):
    side = cols // HALVES
    at = lambda r, z, x: r * cols + z * side + x
    scatter = {o: [] for o in range(1, side)}
    cross, home = [], set()
    for r in range(rows):
        for s in range(STEPS):
            k = (r + s) % rows
            z, x = divmod(k // side, side)
            to = k % side
            offset = (to - x) % side
            if offset:
                scatter[offset].append((at(r, z, x), at(r, z, to)))
            cross.append((at(r, z, to), at(r, 1 - z, to)))
    return scatter, cross


def local(left, right):
    rows, cols = lax.axis_size("row"), lax.axis_size("col")
    size = left.shape[0]
    side = cols // HALVES
    axes = ("row", "col")
    row, col = lax.axis_index("row"), lax.axis_index("col")
    half, x = col // side, col % side
    scatter, cross = routes(rows, cols)
    shift = [((i + 1) % rows, i) for i in range(rows)]
    width = right.shape[1] // CHUNKS

    step = (x - row) % side
    owner = (row + step) % rows // side
    def piece_for(offset):
        return lax.dynamic_slice_in_dim(left, (x + offset) % side * size, size, 1)

    got = piece_for(0)
    for offset, route in scatter.items():
        arrived = lax.ppermute(piece_for(offset), axes, route)
        got = jnp.where((owner % side + offset) % side == x, arrived, got)
    crossed = lax.ppermute(got, axes, cross)
    own = jnp.where(owner // side == half, got, crossed)
    pieces = [own]
    for offset in range(1, side):
        route = [(z * side + (i + offset) % side, z * side + i) for z in range(HALVES) for i in range(side)]
        pieces.append(lax.ppermute(own, "col", route))
    stacked = jnp.concatenate([p[None] for p in pieces], 0)

    outs = []
    chunks = [right[:, i * width:(i + 1) * width] for i in range(CHUNKS)]
    acc = [0.0] * CHUNKS
    for s in range(STEPS):
        block = lax.dynamic_index_in_dim(stacked, (row + s - x) % side, 0, False)
        for i in range(CHUNKS):
            if s:
                chunks[i] = lax.ppermute(chunks[i], "row", shift)
            acc[i] = acc[i] + jnp.dot(block, chunks[i], preferred_element_type=jnp.float32)
    return jnp.concatenate([a.astype(jnp.bfloat16) for a in acc], 1)


def solution(mesh):
    return jax.shard_map(
        local,
        mesh=mesh,
        in_specs=(P("row", "col"), P("row", "col")),
        out_specs=P("row", "col"),
        check_vma=False,
    )
```
